1024 devices in a mesh: gx: 64 (over z_lo, x, core), gy: 16 (over y, z_hi).
Axes of the slice: x: 4, y: 4, z: 32 (z_hi: 4, z_lo: 8; z = z_hi * 8 + z_lo), core: 2. Of those that a mesh axis runs over, the one named last changes fastest.
Arguments:
- prefix_tokens: bfloat16 [49152, 8192], P('gx'), may hold values from -6 to 6
- key_value_weight: bfloat16 [8192, 2048], P('gx', 'gy'), may hold values from -0.0625 to 0.0625
- prefix_lengths: int32 [384], P('gx'), may hold values from 1 to 128, as said below
- start_offsets: int32 [384], P('gx'), may hold values from 0 to 8064
- queries: bfloat16 [32, 8192], P('gy'), may hold values from -5 to 5
- key_value_cache: bfloat16 [2, 32, 8192, 1024], P(None, 'gy', 'gx'), may hold values from -5 to 5
- cache_lengths: int32 [32], P('gy'), may hold values from 1024 to 8192, as said below
- out_weight: bfloat16 [8192, 8192], P('gy', 'gx'), may hold values from -0.5 to 0.5
Outputs:
- prefix_kv: bfloat16 [49152, 2048], P('gx', 'gy')
- decode_out: bfloat16 [32, 8192], P('gy', 'gx')
The draws below stay inside these ranges and needn't reach their ends.
Inputs may be any that keep to these rules, and one draw needn't show every extreme that they name: `prefix_lengths`: live tokens stand at the front of a prefix's slots; in every draw some prefix uses all 128 slots. `cache_lengths`: live positions stand at the front of a trajectory's cache; in every draw some trajectory uses all 8192 positions.
All inputs are finite; a program needn't handle non-finite values.
Results may differ from the reference program's by a relative error of at most 0.0051.
Values may be sent and summed in bfloat16 or wider, within the bound.
A program may use at most 64 MiB of HBM per device.

```python
import jax
import jax.numpy as jnp
from jax import lax

MODEL_WIDTH = 8192
QUERY_HEADS = 64
KEY_VALUE_HEADS = 8
HEAD_SIZE = 128
SLOT = 128
CACHE_PER_SHARD = 128
SEQS = 384
TOKENS = 49152
TRAJECTORY_COUNT = 32
CACHE_LENGTH = 8192
N_GX = 64


def draw_queries(key, part):
    base_key = jax.random.fold_in(key, 21)
    value_rows = jnp.clip(2.0 * jax.random.normal(base_key, (TRAJECTORY_COUNT, QUERY_HEADS * HEAD_SIZE), jnp.float32), -5.0, 5.0)
    return value_rows.astype(jnp.bfloat16)


def draw_key_value_cache(key, part):
    base_key = jax.random.fold_in(key, 22)
    array_shape = (2, TRAJECTORY_COUNT, CACHE_LENGTH, KEY_VALUE_HEADS * HEAD_SIZE)
    value_rows = jnp.clip(jax.random.normal(base_key, array_shape, jnp.float32), -5.0, 5.0)
    return value_rows.astype(jnp.bfloat16)


def draw_cache_lengths(key, part):
    lengths = jax.random.randint(jax.random.fold_in(key, 31), (TRAJECTORY_COUNT,), CACHE_LENGTH // 8, CACHE_LENGTH + 1)
    full_index = jax.random.randint(jax.random.fold_in(key, 32), (), 0, TRAJECTORY_COUNT)
    short_value = jax.random.randint(jax.random.fold_in(key, 33), (), CACHE_LENGTH // 8, CACHE_LENGTH)
    lengths = lengths.at[(full_index + 1) % TRAJECTORY_COUNT].set(short_value)
    return lengths.at[full_index].set(CACHE_LENGTH).astype(jnp.int32)


def draw_prefix_lengths(key, part):
    lengths = jax.random.randint(jax.random.fold_in(key, 41), (SEQS,), 1, SLOT + 1)
    full_index = jax.random.randint(jax.random.fold_in(key, 42), (), 0, SEQS)
    short_value = jax.random.randint(jax.random.fold_in(key, 43), (), 1, SLOT)
    lengths = lengths.at[(full_index + 1) % SEQS].set(short_value)
    return lengths.at[full_index].set(SLOT).astype(jnp.int32)


def plant(entries, stream_key, low, top_value):
    dims = entries.shape
    index_at = [jax.random.randint(jax.random.fold_in(stream_key, axis), (), 0, dims[axis]) for axis in range(len(dims))]
    entries = entries.at[tuple(index_at)].set(low)
    longest = dims.index(max(dims))
    index_at[longest] = (index_at[longest] + 1) % dims[longest]
    return entries.at[tuple(index_at)].set(top_value)


def shard_levels(rng, shape, pieces, least, top_value):
    loudness = 1.0
    for dim, shards_of in pieces:
        heights = jax.random.uniform(jax.random.fold_in(jax.random.fold_in(rng, 6), dim), (shards_of,), jnp.float32, least / len(pieces), top_value / len(pieces))
        loudness = loudness * jnp.repeat(jnp.exp(heights), shape[dim] // shards_of).reshape((-1,) + (1,) * (len(shape) - 1 - dim))
    return loudness


def bell_draw(own_key, extent, spread, limit, shards=(), held_as=jnp.bfloat16):
    array = jax.random.normal(own_key, extent, jnp.float32) * spread
    if len(shards) > 0:
        array = shard_levels(own_key, extent, shards, -0.22, 0.18) * array
    return jnp.clip(array, min=-limit, max=limit).astype(held_as)


def setup_inputs(seed: int = 0) -> dict:
    streams_of = jax.random.split(jax.random.key(seed), 9)
    prefix_tokens = bell_draw(streams_of[0], (TOKENS, MODEL_WIDTH), 1.0, 6.0, ((0, 64),))
    key_value_weight = bell_draw(streams_of[1], (MODEL_WIDTH, 2 * KEY_VALUE_HEADS * HEAD_SIZE), MODEL_WIDTH ** -0.5, 0.0625, ((0, 64), (1, 16)))
    prefix_lengths = draw_prefix_lengths(jax.random.fold_in(streams_of[8], 71), 0)
    start_offsets = plant(jax.random.randint(streams_of[3], (SEQS,), 0, CACHE_LENGTH - SLOT + 1), jax.random.fold_in(streams_of[3], 1), 0, CACHE_LENGTH - SLOT).astype(jnp.int32)
    queries = draw_queries(jax.random.fold_in(streams_of[8], 71), 0)
    key_value_cache = draw_key_value_cache(jax.random.fold_in(streams_of[8], 71), 0)
    cache_lengths = draw_cache_lengths(jax.random.fold_in(streams_of[8], 71), 0)
    out_weight = bell_draw(streams_of[7], (QUERY_HEADS * HEAD_SIZE, MODEL_WIDTH), (QUERY_HEADS * HEAD_SIZE // 64) ** -0.5, 0.5, ((0, 16), (1, 64)))
    return {"prefix_tokens": prefix_tokens, "key_value_weight": key_value_weight, "prefix_lengths": prefix_lengths, "start_offsets": start_offsets, "queries": queries, "key_value_cache": key_value_cache, "cache_lengths": cache_lengths, "out_weight": out_weight}


rope_base = 500000.0
masked_score = -1e30


def rotate_and_mask(projected, first_column, prefix_lengths, start_offsets):
    tok_rows, columns = projected.shape
    slot_index = jnp.arange(SLOT, dtype=jnp.int32)
    positions = (start_offsets[:, None] + slot_index[None, :]).reshape(tok_rows)
    live_rows = (slot_index[None, :] < prefix_lengths[:, None]).reshape(tok_rows)
    half_width = HEAD_SIZE // 2
    freq_index = jnp.arange(half_width, dtype=jnp.float32)
    inverse = rope_base ** (-2.0 * freq_index / HEAD_SIZE)
    angles = positions.astype(jnp.float32)[:, None] * inverse[None, :]
    cosine = jnp.cos(angles)[:, None, :]
    sine = jnp.sin(angles)[:, None, :]
    head_list = projected.reshape(tok_rows, columns // HEAD_SIZE, HEAD_SIZE)
    first_half = head_list[:, :, :half_width]
    second_half = head_list[:, :, half_width:]
    rotary_applied = jnp.concatenate([first_half * cosine - second_half * sine, second_half * cosine + first_half * sine], axis=2)
    head_position = first_column // HEAD_SIZE + jnp.arange(columns // HEAD_SIZE, dtype=jnp.int32)
    key_tagged = jnp.where((head_position < KEY_VALUE_HEADS)[None, :, None], rotary_applied, head_list)
    kept = jnp.where(live_rows[:, None, None], key_tagged, 0.0)
    return kept.reshape(tok_rows, columns).astype(jnp.bfloat16)


def attend_one(query_vector, cache_entry_row, length):
    query_group = QUERY_HEADS // KEY_VALUE_HEADS
    query_head_rows = query_vector.astype(jnp.float32).reshape(KEY_VALUE_HEADS, query_group, HEAD_SIZE)
    key_rows = cache_entry_row[0].astype(jnp.float32).reshape(N_GX, CACHE_PER_SHARD, KEY_VALUE_HEADS, HEAD_SIZE)
    value_rows = cache_entry_row[1].astype(jnp.float32).reshape(N_GX, CACHE_PER_SHARD, KEY_VALUE_HEADS, HEAD_SIZE)
    scores = jnp.einsum("hgd,kphd->khgp", query_head_rows, key_rows, precision=lax.Precision.HIGHEST) * (HEAD_SIZE ** -0.5)
    position = jnp.arange(CACHE_LENGTH, dtype=jnp.int32).reshape(N_GX, 1, 1, CACHE_PER_SHARD)
    valid = position < length
    peak = jnp.max(jnp.where(valid, scores, masked_score), axis=3)
    weights = jnp.where(valid, jnp.exp(scores - peak[..., None]), 0.0)
    block_total = jnp.sum(weights, axis=3)
    rounded = lax.optimization_barrier(weights.astype(jnp.bfloat16)).astype(jnp.float32)
    numerator = jnp.einsum("khgp,kphd->khgd", rounded, value_rows, precision=lax.Precision.HIGHEST)
    highest = jnp.max(peak, axis=0)
    factor = jnp.exp(peak - highest[None])
    denominator = jnp.sum(block_total * factor, axis=0)
    combined = jnp.sum(numerator * factor[..., None], axis=0)
    return (combined / denominator[..., None]).reshape(QUERY_HEADS * HEAD_SIZE).astype(jnp.bfloat16)


def reference(prefix_tokens, key_value_weight, prefix_lengths, start_offsets, queries, key_value_cache, cache_lengths, out_weight):
    projected = jnp.dot(prefix_tokens, key_value_weight, preferred_element_type=jnp.float32)
    prefix_kv = rotate_and_mask(projected, 0, prefix_lengths, start_offsets)

    def one_trajectory(index):
        cache_entry_row = lax.dynamic_index_in_dim(key_value_cache, index, 1, keepdims=False)
        return attend_one(queries[index], cache_entry_row, cache_lengths[index])

    attention = lax.map(one_trajectory, jnp.arange(TRAJECTORY_COUNT, dtype=jnp.int32))
    decode_out = jnp.dot(attention, out_weight, preferred_element_type=jnp.float32).astype(jnp.bfloat16)
    return prefix_kv, decode_out
```

```python
import jax
import jax.numpy as jnp
from jax import lax
from jax.experimental import pallas as pl
from jax.experimental.pallas import tpu as pltpu
from jax.sharding import PartitionSpec as P

QUERY_HEADS = 64
KEY_VALUE_HEADS = 8
HEAD_SIZE = 128
SLOT = 128
NZ, NX, NC, NY, NK = 8, 4, 2, 4, 4
MESH = pl.DeviceIdType.MESH

rope_base = 500000.0
masked_score = -1e30


def device(z, x, c, y, k):
    return ((z * NX + x) * NC + c, y * NK + k)


def merge(nums, metas):
    metas = [m.astype(jnp.float32) for m in metas]
    peaks = [m[:, 0:1] + m[:, 16:17] + m[:, 32:33] for m in metas]
    totals = [m[:, 48:49] + m[:, 64:65] for m in metas]
    top = peaks[0]
    for p in peaks[1:]:
        top = jnp.maximum(top, p)
    num, den = None, None
    for b, p, t in zip(nums, peaks, totals):
        f = jnp.exp(p - top)
        num = b * f if num is None else num + b * f
        den = t * f if den is None else den + t * f
    return top, den, num


def split(v, terms):
    out = []
    for _ in range(terms):
        part = v.astype(jnp.bfloat16)
        out.append(part)
        v = v - part.astype(jnp.float32)
    return out


def meta_of(top, den):
    lane = lax.broadcasted_iota(jnp.int32, (16, 128), 1)
    wide = [t.astype(jnp.float32) for t in split(top, 3) + split(den, 2)]
    meta = jnp.broadcast_to(wide[4], (16, 128))
    for i in (3, 2, 1, 0):
        meta = jnp.where(lane < 16 * (i + 1), wide[i], meta)
    return meta.astype(jnp.bfloat16)


def kernel(
    lens, tok, kvw, q, cache, w,
    proj, dec,
    tokv, kvb, qv, cachev, wall, sbuf, rbuf1, sbuf2, rbuf2, ag, obuf, rob,
    lsem, s1s, s1r, s2s, s2r, as_, ar, bs, br, w1s, w1r, w2s, w2r, zs, zr, xs, xr, cs, cr, os_, or_,
):
    gx = lax.axis_index("gx")
    gy = lax.axis_index("gy")
    z, x, c = gx // 8, (gx // 2) % 4, gx % 2
    y, k = gy // 4, gy % 4
    xc = gx % 8
    up, down = (k + 1) % 4, (k + 3) % 4
    zpeer = [(z + d) % 8 for d in range(1, 8)]
    xcpeer = [(xc + d) % 8 for d in range(1, 8)]
    ypeer = [(y + d) % 4 for d in range(1, 4)]
    xpeer = [(x + d) % 4 for d in range(1, 4)]

    barrier = pltpu.get_barrier_semaphore()
    peers = [device(t, x, c, y, k) for t in zpeer]
    peers += [device(z, t // 2, t % 2, y, k) for t in xcpeer]
    peers += [device(z, x, c, t, k) for t in ypeer]
    peers += [device(z, x, c, y, t) for t in (up, down)]
    for p in peers:
        pl.semaphore_signal(barrier, inc=1, device_id=p, device_id_type=MESH)

    load_q = pltpu.make_async_copy(q, qv, lsem.at[0])
    load_c = pltpu.make_async_copy(cache, cachev, lsem.at[1])
    load_w = pltpu.make_async_copy(w, wall.at[y, pl.ds(0, 512)], lsem.at[2])
    load_k = pltpu.make_async_copy(kvw, kvb.at[z, x, c], lsem.at[3])
    load_t = pltpu.make_async_copy(tok, tokv, lsem.at[4])
    for l in (load_q, load_c, load_w, load_k, load_t):
        l.start()

    load_q.wait()
    load_c.wait()
    q32 = qv[...].astype(jnp.float32)
    row = lax.broadcasted_iota(jnp.int32, (16, 128), 0)
    lane = lax.broadcasted_iota(jnp.int32, (16, 128), 1)
    length = jnp.where(row < 8, lens[0], lens[1])
    valid = gx * 128 + lane < length
    for g in range(8):
        rows = [
            q32[b : b + 1, h * 128 : (h + 1) * 128]
            for b in range(2)
            for h in range(g * 8, g * 8 + 8)
        ]
        q16 = jnp.concatenate(rows, axis=0).astype(jnp.bfloat16)
        cols = slice(g * 128, (g + 1) * 128)
        dn = (((1,), (1,)), ((), ()))
        both = [
            lax.dot_general(q16, cachev[0, b, :, cols], dn, preferred_element_type=jnp.float32)
            for b in range(2)
        ]
        score = jnp.where(row < 8, both[0], both[1]) * HEAD_SIZE ** (-0.5)
        peak = jnp.max(jnp.where(valid, score, masked_score), axis=1, keepdims=True)
        weight = jnp.where(valid, jnp.exp(score - peak), 0.0)
        total = jnp.sum(weight, axis=1, keepdims=True)
        w16 = weight.astype(jnp.bfloat16)
        both = [
            jnp.dot(w16, cachev[1, b, :, cols], preferred_element_type=jnp.float32)
            for b in range(2)
        ]
        sbuf[g, :, :128] = jnp.where(row < 8, both[0], both[1]).astype(jnp.bfloat16)
        sbuf[g, :, 128:] = meta_of(peak, total)

    pl.semaphore_wait(barrier, len(peers))

    def remote(src, dst, ss, rs, dev):
        return pltpu.make_async_remote_copy(
            src_ref=src, dst_ref=dst, send_sem=ss, recv_sem=rs, device_id=dev, device_id_type=MESH
        )

    sends = []

    def go(cp):
        cp.start()
        sends.append(cp)

    for t in zpeer:
        go(remote(sbuf.at[t], rbuf1.at[z], s1s.at[t], s1r.at[z], device(t, x, c, y, k)))
    load_w.wait()
    go(remote(wall.at[y, pl.ds(0, 256)], wall.at[y, pl.ds(512, 256)], w1s.at[0], w1r.at[0], device(z, x, c, y, up)))
    go(remote(wall.at[y, pl.ds(256, 256)], wall.at[y, pl.ds(768, 256)], w1s.at[1], w1r.at[1], device(z, x, c, y, down)))
    for t in ypeer:
        own = wall.at[y, pl.ds(0, 512)]
        go(remote(own, own, w2s.at[0, t], w2r.at[0, y], device(z, x, c, t, k)))
    load_k.wait()
    for t in zpeer:
        own = kvb.at[z, x, c]
        go(remote(own, own, zs.at[t], zr.at[z], device(t, x, c, y, k)))

    here = device(z, x, c, y, k)
    for t in zpeer:
        remote(sbuf.at[t], rbuf1.at[t], s1s.at[t], s1r.at[t], here).wait_recv()
    blocks = [sbuf[z]] + [rbuf1[t] for t in zpeer]
    top, den, num = merge([b[:, :128].astype(jnp.float32) for b in blocks], [b[:, 128:] for b in blocks])
    high, low = split(num, 2)
    sbuf2[:, :128] = high
    sbuf2[:, 128:256] = low
    sbuf2[:, 256:] = meta_of(top, den)
    for t in xcpeer:
        go(remote(sbuf2, rbuf2.at[xc], s2s.at[t], s2r.at[xc], device(z, t // 2, t % 2, y, k)))
    for t in xcpeer:
        remote(sbuf2, rbuf2.at[t], s2s.at[t], s2r.at[t], here).wait_recv()
    blocks = [sbuf2[...]] + [rbuf2[t] for t in xcpeer]
    nums = [b[:, :128].astype(jnp.float32) + b[:, 128:256].astype(jnp.float32) for b in blocks]
    top, den, num = merge(nums, [b[:, 256:] for b in blocks])
    ag[0, z] = (num / den).astype(jnp.bfloat16)

    go(remote(ag.at[0, z], ag.at[1, z], as_.at[0], ar.at[0], device(z, x, c, y, up)))
    go(remote(ag.at[0, z], ag.at[2, z], as_.at[1], ar.at[1], device(z, x, c, y, down)))
    for t in zpeer:
        go(remote(ag.at[0, z], ag.at[0, z], bs.at[0, t], br.at[0, z], device(t, x, c, y, k)))

    for t in zpeer:
        remote(kvb.at[t, x, c], kvb.at[t, x, c], zs.at[t], zr.at[t], here).wait_recv()
    for t in xpeer:
        own = kvb.at[:, x, c]
        go(remote(own, own, xs.at[t], xr.at[x], device(z, t, c, y, k)))

    for s in (1, 2):
        remote(ag.at[0, z], ag.at[s, z], as_.at[s - 1], ar.at[s - 1], here).wait_recv()
        for t in zpeer:
            go(remote(ag.at[s, z], ag.at[s, z], bs.at[s, t], br.at[s, z], device(t, x, c, y, k)))

    for i, lo in ((0, 512), (1, 768)):
        part = wall.at[y, pl.ds(lo, 256)]
        remote(part, part, w1s.at[i], w1r.at[i], here).wait_recv()
    for t in ypeer:
        part = wall.at[y, pl.ds(512, 512)]
        go(remote(part, part, w2s.at[1, t], w2r.at[1, y], device(z, x, c, t, k)))

    for t in xpeer:
        part = kvb.at[:, t, c]
        remote(part, part, xs.at[t], xr.at[t], here).wait_recv()
    own = kvb.at[:, :, c]
    go(remote(own, own, cs, cr, device(z, x, 1 - c, y, k)))

    for s in range(3):
        for t in zpeer:
            remote(ag.at[s, t], ag.at[s, t], bs.at[s, t], br.at[s, t], here).wait_recv()
    for i in range(2):
        for t in ypeer:
            part = wall.at[t, pl.ds(512 * i, 512)]
            remote(part, part, w2s.at[i, t], w2r.at[i, t], here).wait_recv()

    row16 = lax.broadcasted_iota(jnp.int32, (16, 128), 0) % 8
    zero = jnp.zeros((16, 128), jnp.bfloat16)
    acc = jnp.zeros((48, 128), jnp.float32)
    for yy in range(4):
        cols = []
        for d, r in ((0, 0), (0, 1), (0, 2), (0, 3), (3, 0), (3, 1), (1, 2), (1, 3)):
            zh = (k + d) % 4
            keep = row16 == (zh % 2) * 4 + r
            use = {(0, 0): (0, 1), (0, 1): (0, 1), (0, 2): (0, 2), (0, 3): (0, 2)}.get((d, r))
            use = use or ((0, 2) if d == 3 else (0, 1))
            col = []
            for s in range(3):
                if s in use:
                    tile = ag[s, 2 * yy + zh // 2].astype(jnp.float32)
                    col.append(jnp.where(keep, tile, 0.0).astype(jnp.bfloat16))
                else:
                    col.append(zero)
            cols.append(jnp.concatenate(col, axis=0))
        lhs = jnp.concatenate(cols, axis=1)
        acc += jnp.dot(lhs, wall[yy], preferred_element_type=jnp.float32)
    sums = [jnp.sum(acc[8 * i : 8 * i + 8], axis=0, keepdims=True) for i in range(6)]
    obuf[...] = jnp.concatenate(sums + [jnp.zeros((2, 128), jnp.float32)], axis=0)
    go(remote(obuf, rob.at[0], os_.at[0], or_.at[0], device(z, x, c, y, down)))
    go(remote(obuf, rob.at[1], os_.at[1], or_.at[1], device(z, x, c, y, up)))

    other = kvb.at[:, :, 1 - c]
    remote(other, other, cs, cr, here).wait_recv()
    load_t.wait()
    proj[...] = jnp.zeros_like(proj)

    @pl.loop(0, 8)
    def _(i):
        lhs = tokv[:, pl.ds(pl.multiple_of(i * 1024, 1024), 1024)]
        rhs = kvb[i].reshape(1024, 128)
        proj[...] += jnp.dot(lhs, rhs, preferred_element_type=jnp.float32)

    for i in range(2):
        remote(obuf, rob.at[i], os_.at[i], or_.at[i], here).wait_recv()
    dec[0:2] = obuf[0:2] + rob[0, 2:4] + rob[1, 4:6]
    for s in sends:
        s.wait_send()


def rotate_and_mask(projected, is_key, prefix_lengths, start_offsets):
    tok_rows = projected.shape[0]
    slot_index = jnp.arange(SLOT, dtype=jnp.int32)
    positions = (start_offsets[:, None] + slot_index[None, :]).reshape(tok_rows)
    live_rows = (slot_index[None, :] < prefix_lengths[:, None]).reshape(tok_rows)
    half_width = HEAD_SIZE // 2
    freq_index = jnp.arange(half_width, dtype=jnp.float32)
    inverse = rope_base ** (-2.0 * freq_index / HEAD_SIZE)
    angles = positions.astype(jnp.float32)[:, None] * inverse[None, :]
    cosine = jnp.cos(angles)
    sine = jnp.sin(angles)
    first_half = projected[:, :half_width]
    second_half = projected[:, half_width:]
    rotated = jnp.concatenate(
        [first_half * cosine - second_half * sine, second_half * cosine + first_half * sine], axis=1
    )
    kept = jnp.where(live_rows[:, None], jnp.where(is_key, rotated, projected), 0.0)
    return kept.astype(jnp.bfloat16)


def shards(tok, kvw, prefix_lengths, start_offsets, q, cache, lens, w):
    bf, f32 = jnp.bfloat16, jnp.float32
    vm = pltpu.VMEM
    dma = pltpu.SemaphoreType.DMA
    any_ = pl.BlockSpec(memory_space=pl.ANY)
    vmem = pl.BlockSpec(memory_space=pltpu.VMEM)
    proj, dec = pl.pallas_call(
        kernel,
        out_shape=(jax.ShapeDtypeStruct((tok.shape[0], 128), f32), jax.ShapeDtypeStruct((2, 128), f32)),
        in_specs=[pl.BlockSpec(memory_space=pltpu.SMEM)] + [any_] * 5,
        out_specs=(vmem, vmem),
        scratch_shapes=[
            vm(tok.shape, bf), vm((8, 4, 2, 128, 128), bf), vm(q.shape, bf), vm(cache.shape, bf),
            vm((4, 1024, 128), bf), vm((8, 16, 256), bf), vm((8, 16, 256), bf), vm((16, 384), bf),
            vm((8, 16, 384), bf), vm((3, 8, 16, 128), bf), vm((8, 128), f32), vm((2, 8, 128), f32),
            dma((5,)), dma((8,)), dma((8,)), dma((8,)), dma((8,)), dma((2,)), dma((2,)),
            dma((3, 8)), dma((3, 8)), dma((2,)), dma((2,)), dma((2, 4)), dma((2, 4)),
            dma((8,)), dma((8,)), dma((4,)), dma((4,)), dma, dma, dma((2,)), dma((2,)),
        ],
        compiler_params=pltpu.CompilerParams(
            collective_id=0, has_side_effects=True, vmem_limit_bytes=40 * 1024 * 1024
        ),
    )(lens, tok, kvw, q, cache, w)
    is_key = lax.axis_index("gy") < KEY_VALUE_HEADS
    return rotate_and_mask(proj, is_key, prefix_lengths, start_offsets), dec.astype(jnp.bfloat16)


def solution(mesh):
    return jax.shard_map(
        shards,
        mesh=mesh,
        in_specs=(
            P("gx", None), P("gx", "gy"), P("gx"), P("gx"), P("gy", None),
            P(None, "gy", "gx", None), P("gy"), P("gy", "gx"),
        ),
        out_specs=(P("gx", "gy"), P("gy", "gx")),
        check_vma=False,
    )
```

```python
import jax
import jax.numpy as jnp
import numpy as np
from jax import lax
from jax.experimental import pallas as pl
from jax.experimental.pallas import tpu as pltpu
from jax.sharding import PartitionSpec as P

QUERY_HEADS = 64
KEY_VALUE_HEADS = 8
HEAD_SIZE = 128
SLOT = 128
NZ, NX, NC, NY, NK = 8, 4, 2, 4, 4
MESH = pl.DeviceIdType.MESH

rope_base = 500000.0
masked_score = -1e30


def device(z, x, c, y, k):
    return ((z * NX + x) * NC + c, y * NK + k)


def merge(nums, metas):
    metas = [m.astype(jnp.float32) for m in metas]
    peaks = [m[:, 0:1] + m[:, 16:17] + m[:, 32:33] for m in metas]
    totals = [m[:, 48:49] + m[:, 64:65] for m in metas]
    top = peaks[0]
    for p in peaks[1:]:
        top = jnp.maximum(top, p)
    num, den = None, None
    for b, p, t in zip(nums, peaks, totals):
        f = jnp.exp(p - top)
        num = b * f if num is None else num + b * f
        den = t * f if den is None else den + t * f
    return top, den, num


def split(v, terms):
    out = []
    for _ in range(terms):
        part = v.astype(jnp.bfloat16)
        out.append(part)
        v = v - part.astype(jnp.float32)
    return out


def meta_of(top, den):
    lane = lax.broadcasted_iota(jnp.int32, (16, 128), 1)
    wide = [t.astype(jnp.float32) for t in split(top, 3) + split(den, 2)]
    meta = jnp.broadcast_to(wide[4], (16, 128))
    for i in (3, 2, 1, 0):
        meta = jnp.where(lane < 16 * (i + 1), wide[i], meta)
    return meta.astype(jnp.bfloat16)


def turn(angle):
    n = jnp.floor(angle * (2.0 / np.pi) + 0.5)
    r = angle - n * 1.5703125
    r = r - n * 4.837512969970703125e-4
    r = r - n * 7.54978995489188216e-8
    z = r * r
    s = ((-1.9515295891e-4 * z + 8.3321608736e-3) * z - 1.6666654611e-1) * z * r + r
    c = ((2.443315711809948e-5 * z - 1.388731625493765e-3) * z + 4.166664568298827e-2) * z * z - 0.5 * z + 1.0
    quarter = n - 4.0 * jnp.floor(n * 0.25)
    odd = (quarter == 1.0) | (quarter == 3.0)
    cosine = jnp.where(odd, s, c)
    sine = jnp.where(odd, c, s)
    cosine = jnp.where((quarter == 1.0) | (quarter == 2.0), -cosine, cosine)
    sine = jnp.where(quarter >= 2.0, -sine, sine)
    return cosine, sine


def kernel(
    lens, plen, start, inv, tok, kvw, q, cache, w,
    kv_out, dec,
    proj, cos_t, sin_t, tokv, kvb, qv, cachev, wall, sbuf, rbuf1, sbuf2, rbuf2, ag, obuf, rob,
    lsem, s1s, s1r, s2s, s2r, as_, ar, bs, br, w1s, w1r, w2s, w2r, zs, zr, xs, xr, cs, cr, os_, or_, far,
):
    gx = lax.axis_index("gx")
    gy = lax.axis_index("gy")
    z, x, c = gx // 8, (gx // 2) % 4, gx % 2
    y, k = gy // 4, gy % 4
    xc = gx % 8
    up, down = (k + 1) % 4, (k + 3) % 4
    zpeer = [(z + d) % 8 for d in range(1, 8)]
    xcpeer = [(xc + d) % 8 for d in range(1, 8)]
    ypeer = [(y + d) % 4 for d in range(1, 4)]
    xpeer = [(x + d) % 4 for d in range(1, 4)]

    barrier = pltpu.get_barrier_semaphore()
    peers = [device(t, x, c, y, k) for t in zpeer]
    peers += [device(z, t // 2, t % 2, y, k) for t in xcpeer]
    peers += [device(z, x, c, t, k) for t in ypeer]
    for p in peers:
        pl.semaphore_signal(barrier, inc=1, device_id=p, device_id_type=MESH)
    first, last = z == 0, z == NZ - 1
    above, below = device(0, x, c, y, up), device(NZ - 1, x, c, y, down)

    @pl.when(last)
    def _():
        pl.semaphore_signal(barrier, inc=1, device_id=above, device_id_type=MESH)

    @pl.when(first)
    def _():
        pl.semaphore_signal(barrier, inc=1, device_id=below, device_id_type=MESH)

    load_q = pltpu.make_async_copy(q, qv, lsem.at[0])
    load_c = pltpu.make_async_copy(cache, cachev, lsem.at[1])
    load_w = pltpu.make_async_copy(w, wall.at[y, pl.ds(0, 512)], lsem.at[2])
    load_k = pltpu.make_async_copy(kvw, kvb.at[z, x, c], lsem.at[3])
    load_t = pltpu.make_async_copy(tok, tokv, lsem.at[4])
    for l in (load_q, load_c, load_w, load_k, load_t):
        l.start()

    load_q.wait()
    load_c.wait()
    q32 = qv[...].astype(jnp.float32)
    row = lax.broadcasted_iota(jnp.int32, (16, 128), 0)
    lane = lax.broadcasted_iota(jnp.int32, (16, 128), 1)
    length = jnp.where(row < 8, lens[0], lens[1])
    valid = gx * 128 + lane < length
    for g in range(8):
        rows = [
            q32[b : b + 1, h * 128 : (h + 1) * 128]
            for b in range(2)
            for h in range(g * 8, g * 8 + 8)
        ]
        q16 = jnp.concatenate(rows, axis=0).astype(jnp.bfloat16)
        cols = slice(g * 128, (g + 1) * 128)
        dn = (((1,), (1,)), ((), ()))
        both = [
            lax.dot_general(q16, cachev[0, b, :, cols], dn, preferred_element_type=jnp.float32)
            for b in range(2)
        ]
        score = jnp.where(row < 8, both[0], both[1]) * HEAD_SIZE ** (-0.5)
        peak = jnp.max(jnp.where(valid, score, masked_score), axis=1, keepdims=True)
        weight = jnp.where(valid, jnp.exp(score - peak), 0.0)
        total = jnp.sum(weight, axis=1, keepdims=True)
        w16 = weight.astype(jnp.bfloat16)
        both = [
            jnp.dot(w16, cachev[1, b, :, cols], preferred_element_type=jnp.float32)
            for b in range(2)
        ]
        sbuf[g, :, :128] = jnp.where(row < 8, both[0], both[1]).astype(jnp.bfloat16)
        sbuf[g, :, 128:] = meta_of(peak, total)

    sign = jnp.where(lax.broadcasted_iota(jnp.int32, (SLOT, 128), 1) < 64, -1.0, 1.0)
    slot = lax.broadcasted_iota(jnp.int32, (SLOT, 128), 0)
    for i in range(plen.shape[0]):
        angle = (start[i] + slot).astype(jnp.float32) * inv[...]
        cosine, sine = turn(angle)
        cos_t[i * SLOT : (i + 1) * SLOT] = cosine
        sin_t[i * SLOT : (i + 1) * SLOT] = sine * sign

    pl.semaphore_wait(barrier, len(peers) + (z + 6) // 13 + (NZ - z) // NZ)

    @pl.when(last)
    def _():
        pl.semaphore_signal(far.at[0], inc=1, device_id=above, device_id_type=MESH)

    @pl.when(first)
    def _():
        pl.semaphore_signal(far.at[1], inc=1, device_id=below, device_id_type=MESH)

    def remote(src, dst, ss, rs, dev):
        return pltpu.make_async_remote_copy(
            src_ref=src, dst_ref=dst, send_sem=ss, recv_sem=rs, device_id=dev, device_id_type=MESH
        )

    sends = []

    def go(cp):
        cp.start()
        sends.append(cp)

    for t in zpeer:
        go(remote(sbuf.at[t], rbuf1.at[z], s1s.at[t], s1r.at[z], device(t, x, c, y, k)))
    load_k.wait()
    for t in zpeer:
        own = kvb.at[z, x, c]
        go(remote(own, own, zs.at[t], zr.at[z], device(t, x, c, y, k)))

    load_w.wait()
    for t in ypeer:
        own = wall.at[y, pl.ds(0, 512)]
        go(remote(own, own, w2s.at[0, t], w2r.at[0, y], device(z, x, c, t, k)))

    for flag, end in ((0, first), (1, last)):

        @pl.when(end)
        def _():
            pl.semaphore_wait(far.at[flag], 1)
            for t in zpeer:
                pl.semaphore_signal(far.at[flag], inc=1, device_id=device(t, x, c, y, k), device_id_type=MESH)

    here = device(z, x, c, y, k)
    for t in zpeer:
        remote(sbuf.at[t], rbuf1.at[t], s1s.at[t], s1r.at[t], here).wait_recv()
    for flag, end in ((0, first), (1, last)):

        @pl.when(jnp.logical_not(end))
        def _():
            pl.semaphore_wait(far.at[flag], 1)

    go(remote(wall.at[y, pl.ds(0, 256)], wall.at[y, pl.ds(512, 256)], w1s.at[0], w1r.at[0], device(z, x, c, y, up)))
    go(remote(wall.at[y, pl.ds(256, 256)], wall.at[y, pl.ds(768, 256)], w1s.at[1], w1r.at[1], device(z, x, c, y, down)))
    blocks = [sbuf[z]] + [rbuf1[t] for t in zpeer]
    top, den, num = merge([b[:, :128].astype(jnp.float32) for b in blocks], [b[:, 128:] for b in blocks])
    high, low = split(num, 2)
    sbuf2[:, :128] = high
    sbuf2[:, 128:256] = low
    sbuf2[:, 256:] = meta_of(top, den)
    for t in xcpeer:
        go(remote(sbuf2, rbuf2.at[xc], s2s.at[t], s2r.at[xc], device(z, t // 2, t % 2, y, k)))
    for t in xcpeer:
        remote(sbuf2, rbuf2.at[t], s2s.at[t], s2r.at[t], here).wait_recv()
    blocks = [sbuf2[...]] + [rbuf2[t] for t in xcpeer]
    nums = [b[:, :128].astype(jnp.float32) + b[:, 128:256].astype(jnp.float32) for b in blocks]
    top, den, num = merge(nums, [b[:, 256:] for b in blocks])
    ag[0, z] = (num / den).astype(jnp.bfloat16)

    go(remote(ag.at[0, z], ag.at[1, z], as_.at[0], ar.at[0], device(z, x, c, y, up)))
    go(remote(ag.at[0, z], ag.at[2, z], as_.at[1], ar.at[1], device(z, x, c, y, down)))
    for t in zpeer:
        go(remote(ag.at[0, z], ag.at[0, z], bs.at[0, t], br.at[0, z], device(t, x, c, y, k)))

    for t in zpeer:
        remote(kvb.at[t, x, c], kvb.at[t, x, c], zs.at[t], zr.at[t], here).wait_recv()
    for t in xpeer:
        own = kvb.at[:, x, c]
        go(remote(own, own, xs.at[t], xr.at[x], device(z, t, c, y, k)))

    for i, lo in ((0, 512), (1, 768)):
        part = wall.at[y, pl.ds(lo, 256)]
        remote(part, part, w1s.at[i], w1r.at[i], here).wait_recv()
    for t in ypeer:
        part = wall.at[y, pl.ds(512, 512)]
        go(remote(part, part, w2s.at[1, t], w2r.at[1, y], device(z, x, c, t, k)))

    for s in (1, 2):
        remote(ag.at[0, z], ag.at[s, z], as_.at[s - 1], ar.at[s - 1], here).wait_recv()
        for t in zpeer:
            go(remote(ag.at[s, z], ag.at[s, z], bs.at[s, t], br.at[s, z], device(t, x, c, y, k)))

    for t in xpeer:
        part = kvb.at[:, t, c]
        remote(part, part, xs.at[t], xr.at[t], here).wait_recv()
    own = kvb.at[:, :, c]
    go(remote(own, own, cs, cr, device(z, x, 1 - c, y, k)))

    for s in range(3):
        for t in zpeer:
            remote(ag.at[s, t], ag.at[s, t], bs.at[s, t], br.at[s, t], here).wait_recv()
    for i in range(2):
        for t in ypeer:
            part = wall.at[t, pl.ds(512 * i, 512)]
            remote(part, part, w2s.at[i, t], w2r.at[i, t], here).wait_recv()

    row16 = lax.broadcasted_iota(jnp.int32, (16, 128), 0) % 8
    zero = jnp.zeros((16, 128), jnp.bfloat16)
    acc = jnp.zeros((48, 128), jnp.float32)
    for yy in range(4):
        cols = []
        for d, r in ((0, 0), (0, 1), (0, 2), (0, 3), (3, 0), (3, 1), (1, 2), (1, 3)):
            zh = (k + d) % 4
            keep = row16 == (zh % 2) * 4 + r
            use = {(0, 0): (0, 1), (0, 1): (0, 1), (0, 2): (0, 2), (0, 3): (0, 2)}.get((d, r))
            use = use or ((0, 2) if d == 3 else (0, 1))
            col = []
            for s in range(3):
                if s in use:
                    tile = ag[s, 2 * yy + zh // 2].astype(jnp.float32)
                    col.append(jnp.where(keep, tile, 0.0).astype(jnp.bfloat16))
                else:
                    col.append(zero)
            cols.append(jnp.concatenate(col, axis=0))
        lhs = jnp.concatenate(cols, axis=1)
        acc += jnp.dot(lhs, wall[yy], preferred_element_type=jnp.float32)
    sums = [jnp.sum(acc[8 * i : 8 * i + 8], axis=0, keepdims=True) for i in range(6)]
    obuf[...] = jnp.concatenate(sums + [jnp.zeros((2, 128), jnp.float32)], axis=0)
    go(remote(obuf, rob.at[0], os_.at[0], or_.at[0], device(z, x, c, y, down)))
    go(remote(obuf, rob.at[1], os_.at[1], or_.at[1], device(z, x, c, y, up)))

    other = kvb.at[:, :, 1 - c]
    remote(other, other, cs, cr, here).wait_recv()
    load_t.wait()
    proj[...] = jnp.zeros_like(proj)

    @pl.loop(0, 8)
    def _(i):
        lhs = tokv[:, pl.ds(pl.multiple_of(i * 1024, 1024), 1024)]
        rhs = kvb[i].reshape(1024, 128)
        proj[...] += jnp.dot(lhs, rhs, preferred_element_type=jnp.float32)

    is_key = gy < KEY_VALUE_HEADS
    for i in range(plen.shape[0]):
        rows = slice(i * SLOT, (i + 1) * SLOT)
        plain = proj[rows]
        turned = plain * cos_t[rows] + pltpu.roll(plain, 64, 1) * sin_t[rows]
        kept = jnp.where(slot < plen[i], jnp.where(is_key, turned, plain), 0.0)
        kv_out[rows] = kept.astype(jnp.bfloat16)

    for i in range(2):
        remote(obuf, rob.at[i], os_.at[i], or_.at[i], here).wait_recv()
    dec[...] = (obuf[0:2] + rob[0, 2:4] + rob[1, 4:6]).astype(jnp.bfloat16)
    for s in sends:
        s.wait_send()


def shards(tok, kvw, prefix_lengths, start_offsets, q, cache, lens, w):
    bf, f32 = jnp.bfloat16, jnp.float32
    vm = pltpu.VMEM
    dma = pltpu.SemaphoreType.DMA
    hbm = pl.BlockSpec(memory_space=pltpu.HBM)
    smem = pl.BlockSpec(memory_space=pltpu.SMEM)
    vmem = pl.BlockSpec(memory_space=pltpu.VMEM)
    inverse = rope_base ** (-2.0 * (np.arange(128) % 64) / HEAD_SIZE)
    prefix_kv, dec = pl.pallas_call(
        kernel,
        out_shape=(jax.ShapeDtypeStruct((tok.shape[0], 128), bf), jax.ShapeDtypeStruct((2, 128), bf)),
        in_specs=[smem] * 3 + [vmem] + [hbm] * 5,
        out_specs=(vmem, vmem),
        scratch_shapes=[
            vm((tok.shape[0], 128), f32), vm((tok.shape[0], 128), f32), vm((tok.shape[0], 128), f32),
            vm(tok.shape, bf), vm((8, 4, 2, 128, 128), bf), vm(q.shape, bf), vm(cache.shape, bf),
            vm((4, 1024, 128), bf), vm((8, 16, 256), bf), vm((8, 16, 256), bf), vm((16, 384), bf),
            vm((8, 16, 384), bf), vm((3, 8, 16, 128), bf), vm((8, 128), f32), vm((2, 8, 128), f32),
            dma((5,)), dma((8,)), dma((8,)), dma((8,)), dma((8,)), dma((2,)), dma((2,)),
            dma((3, 8)), dma((3, 8)), dma((2,)), dma((2,)), dma((2, 4)), dma((2, 4)),
            dma((8,)), dma((8,)), dma((4,)), dma((4,)), dma, dma, dma((2,)), dma((2,)),
            pltpu.SemaphoreType.REGULAR((2,)),
        ],
        compiler_params=pltpu.CompilerParams(
            collective_id=0, has_side_effects=True, vmem_limit_bytes=67043328
        ),
    )(lens, prefix_lengths, start_offsets, np.float32(inverse)[None, :], tok, kvw, q, cache, w)
    return prefix_kv, dec


def solution(mesh):
    return jax.shard_map(
        shards,
        mesh=mesh,
        in_specs=(
            P("gx", None), P("gx", "gy"), P("gx"), P("gx"), P("gy", None),
            P(None, "gy", "gx", None), P("gy"), P("gy", "gx"),
        ),
        out_specs=(P("gx", "gy"), P("gy", "gx")),
        check_vma=False,
    )
```

```python
import jax
import jax.numpy as jnp
import numpy as np
from jax import lax
from jax.experimental import pallas as pl
from jax.experimental.pallas import tpu as pltpu
from jax.sharding import PartitionSpec as P

QUERY_HEADS = 64
KEY_VALUE_HEADS = 8
HEAD_SIZE = 128
SLOT = 128
NZ, NX, NC, NY, NK = 8, 4, 2, 4, 4
MESH = pl.DeviceIdType.MESH

rope_base = 500000.0
masked_score = -1e30


def device(z, x, c, y, k):
    return ((z * NX + x) * NC + c, y * NK + k)


def merge(nums, metas):
    metas = [m.astype(jnp.float32) for m in metas]
    peaks = [m[:, 0:1] + m[:, 16:17] + m[:, 32:33] for m in metas]
    totals = [m[:, 48:49] + m[:, 64:65] for m in metas]
    top = peaks[0]
    for p in peaks[1:]:
        top = jnp.maximum(top, p)
    num, den = None, None
    for b, p, t in zip(nums, peaks, totals):
        f = jnp.exp(p - top)
        num = b * f if num is None else num + b * f
        den = t * f if den is None else den + t * f
    return top, den, num


def split(v, terms):
    out = []
    for _ in range(terms):
        part = v.astype(jnp.bfloat16)
        out.append(part)
        v = v - part.astype(jnp.float32)
    return out


def meta_of(top, den):
    lane = lax.broadcasted_iota(jnp.int32, (16, 128), 1)
    wide = [t.astype(jnp.float32) for t in split(top, 3) + split(den, 2)]
    meta = jnp.broadcast_to(wide[4], (16, 128))
    for i in (3, 2, 1, 0):
        meta = jnp.where(lane < 16 * (i + 1), wide[i], meta)
    return meta.astype(jnp.bfloat16)


def turn(angle):
    n = jnp.floor(angle * (2.0 / np.pi) + 0.5)
    r = angle - n * 1.5703125
    r = r - n * 4.837512969970703125e-4
    r = r - n * 7.54978995489188216e-8
    z = r * r
    s = ((-1.9515295891e-4 * z + 8.3321608736e-3) * z - 1.6666654611e-1) * z * r + r
    c = ((2.443315711809948e-5 * z - 1.388731625493765e-3) * z + 4.166664568298827e-2) * z * z - 0.5 * z + 1.0
    quarter = n - 4.0 * jnp.floor(n * 0.25)
    odd = (quarter == 1.0) | (quarter == 3.0)
    cosine = jnp.where(odd, s, c)
    sine = jnp.where(odd, c, s)
    cosine = jnp.where((quarter == 1.0) | (quarter == 2.0), -cosine, cosine)
    sine = jnp.where(quarter >= 2.0, -sine, sine)
    return cosine, sine


def kernel(
    lens, plen, start, inv, tok, kvw, q, cache, w,
    kv_out, dec,
    proj, cos_t, sin_t, tokv, kvb, qv, cachev, wall, sbuf, rbuf1, sbuf2, rbuf2, ag, obuf, rob,
    lsem, s1s, s1r, s2s, s2r, as_, ar, bs, br, w1s, w1r, w2s, w2r, zs, zr, xs, xr, cs, cr, os_, or_, far,
):
    gx = lax.axis_index("gx")
    gy = lax.axis_index("gy")
    z, x, c = gx // 8, (gx // 2) % 4, gx % 2
    y, k = gy // 4, gy % 4
    xc = gx % 8
    up, down = (k + 1) % 4, (k + 3) % 4
    zpeer = [(z + d) % 8 for d in range(1, 8)]
    xcpeer = [(xc + d) % 8 for d in range(1, 8)]
    ypeer = [(y + d) % 4 for d in range(1, 4)]
    xpeer = [(x + d) % 4 for d in range(1, 4)]

    barrier = pltpu.get_barrier_semaphore()
    peers = [device(t, x, c, y, k) for t in zpeer]
    peers += [device(z, t // 2, t % 2, y, k) for t in xcpeer]
    peers += [device(z, x, c, t, k) for t in ypeer]
    for p in peers:
        pl.semaphore_signal(barrier, inc=1, device_id=p, device_id_type=MESH)
    first, last = z == 0, z == NZ - 1
    above, below = device(0, x, c, y, up), device(NZ - 1, x, c, y, down)

    @pl.when(last)
    def _():
        pl.semaphore_signal(barrier, inc=1, device_id=above, device_id_type=MESH)

    @pl.when(first)
    def _():
        pl.semaphore_signal(barrier, inc=1, device_id=below, device_id_type=MESH)

    load_q = pltpu.make_async_copy(q, qv, lsem.at[0])
    load_c = pltpu.make_async_copy(cache, cachev, lsem.at[1])
    load_w = pltpu.make_async_copy(w, wall.at[y, pl.ds(0, 512)], lsem.at[2])
    load_k = pltpu.make_async_copy(kvw, kvb.at[z, x, c], lsem.at[3])
    load_t = pltpu.make_async_copy(tok, tokv, lsem.at[4])
    for l in (load_q, load_c, load_k, load_w):
        l.start()

    load_q.wait()
    load_c.wait()
    load_t.start()
    q32 = qv[...].astype(jnp.float32)
    row = lax.broadcasted_iota(jnp.int32, (16, 128), 0)
    lane = lax.broadcasted_iota(jnp.int32, (16, 128), 1)
    length = jnp.where(row < 8, lens[0], lens[1])
    valid = gx * 128 + lane < length
    for g in range(8):
        rows = [
            q32[b : b + 1, h * 128 : (h + 1) * 128]
            for b in range(2)
            for h in range(g * 8, g * 8 + 8)
        ]
        q16 = jnp.concatenate(rows, axis=0).astype(jnp.bfloat16)
        cols = slice(g * 128, (g + 1) * 128)
        dn = (((1,), (1,)), ((), ()))
        both = [
            lax.dot_general(q16, cachev[0, b, :, cols], dn, preferred_element_type=jnp.float32)
            for b in range(2)
        ]
        score = jnp.where(row < 8, both[0], both[1]) * HEAD_SIZE ** (-0.5)
        peak = jnp.max(jnp.where(valid, score, masked_score), axis=1, keepdims=True)
        weight = jnp.where(valid, jnp.exp(score - peak), 0.0)
        total = jnp.sum(weight, axis=1, keepdims=True)
        w16 = weight.astype(jnp.bfloat16)
        both = [
            jnp.dot(w16, cachev[1, b, :, cols], preferred_element_type=jnp.float32)
            for b in range(2)
        ]
        sbuf[g, :, :128] = jnp.where(row < 8, both[0], both[1]).astype(jnp.bfloat16)
        sbuf[g, :, 128:] = meta_of(peak, total)

    pl.semaphore_wait(barrier, len(peers) + (z + 6) // 13 + (NZ - z) // NZ)

    @pl.when(last)
    def _():
        pl.semaphore_signal(far.at[0], inc=1, device_id=above, device_id_type=MESH)

    @pl.when(first)
    def _():
        pl.semaphore_signal(far.at[1], inc=1, device_id=below, device_id_type=MESH)

    def remote(src, dst, ss, rs, dev):
        return pltpu.make_async_remote_copy(
            src_ref=src, dst_ref=dst, send_sem=ss, recv_sem=rs, device_id=dev, device_id_type=MESH
        )

    sends = []

    def go(cp):
        cp.start()
        sends.append(cp)

    for t in zpeer:
        go(remote(sbuf.at[t], rbuf1.at[z], s1s.at[t], s1r.at[z], device(t, x, c, y, k)))
    load_k.wait()
    mate = (z + 4) % 8
    quad = [z // 4 * 4 + (z + d) % 4 for d in range(1, 4)]
    far_quad = [mate // 4 * 4 + (z + d) % 4 for d in range(1, 4)]
    own = kvb.at[z, x, c]
    for t in [mate] + quad:
        go(remote(own, own, zs.at[t], zr.at[z], device(t, x, c, y, k)))
    for u in xpeer:
        own = kvb.at[z, x, c]
        go(remote(own, own, xs.at[z, u], xr.at[z, x], device(z, u, c, y, k)))

    for flag, end in ((0, first), (1, last)):

        @pl.when(end)
        def _():
            pl.semaphore_wait(far.at[flag], 1)
            for t in zpeer:
                pl.semaphore_signal(far.at[flag], inc=1, device_id=device(t, x, c, y, k), device_id_type=MESH)

    for flag, end in ((0, first), (1, last)):

        @pl.when(jnp.logical_not(end))
        def _():
            pl.semaphore_wait(far.at[flag], 1)

    load_w.wait()
    go(remote(wall.at[y, pl.ds(0, 256)], wall.at[y, pl.ds(512, 256)], w1s.at[0], w1r.at[0], device(z, x, c, y, up)))
    go(remote(wall.at[y, pl.ds(256, 256)], wall.at[y, pl.ds(768, 256)], w1s.at[1], w1r.at[1], device(z, x, c, y, down)))
    for t in ypeer:
        own = wall.at[y, pl.ds(0, 512)]
        go(remote(own, own, w2s.at[0, t], w2r.at[0, y], device(z, x, c, t, k)))

    sign = jnp.where(lax.broadcasted_iota(jnp.int32, (SLOT, 128), 1) < 64, -1.0, 1.0)
    slot = lax.broadcasted_iota(jnp.int32, (SLOT, 128), 0)
    for i in range(plen.shape[0]):
        angle = (start[i] + slot).astype(jnp.float32) * inv[...]
        cosine, sine = turn(angle)
        cos_t[i * SLOT : (i + 1) * SLOT] = cosine
        sin_t[i * SLOT : (i + 1) * SLOT] = sine * sign

    here = device(z, x, c, y, k)
    for t in zpeer:
        remote(sbuf.at[t], rbuf1.at[t], s1s.at[t], s1r.at[t], here).wait_recv()
    blocks = [sbuf[z]] + [rbuf1[t] for t in zpeer]
    top, den, num = merge([b[:, :128].astype(jnp.float32) for b in blocks], [b[:, 128:] for b in blocks])
    high, low = split(num, 2)
    sbuf2[:, :128] = high
    sbuf2[:, 128:256] = low
    sbuf2[:, 256:] = meta_of(top, den)
    for t in xcpeer:
        go(remote(sbuf2, rbuf2.at[xc], s2s.at[t], s2r.at[xc], device(z, t // 2, t % 2, y, k)))
    part = kvb.at[mate, x, c]
    remote(part, part, zs.at[mate], zr.at[mate], here).wait_recv()
    for t, u in zip(quad, far_quad):
        go(remote(part, part, zs.at[u], zr.at[mate], device(t, x, c, y, k)))
    for u in xpeer:
        go(remote(part, part, xs.at[mate, u], xr.at[mate, x], device(z, u, c, y, k)))
    for t in quad:
        part = kvb.at[t, x, c]
        remote(part, part, zs.at[t], zr.at[t], here).wait_recv()
        for u in xpeer:
            go(remote(part, part, xs.at[t, u], xr.at[t, x], device(z, u, c, y, k)))
    for t in xcpeer:
        remote(sbuf2, rbuf2.at[t], s2s.at[t], s2r.at[t], here).wait_recv()
    blocks = [sbuf2[...]] + [rbuf2[t] for t in xcpeer]
    nums = [b[:, :128].astype(jnp.float32) + b[:, 128:256].astype(jnp.float32) for b in blocks]
    top, den, num = merge(nums, [b[:, 256:] for b in blocks])
    ag[0, z] = (num / den).astype(jnp.bfloat16)

    go(remote(ag.at[0, z], ag.at[1, z], as_.at[0], ar.at[0], device(z, x, c, y, up)))
    go(remote(ag.at[0, z], ag.at[2, z], as_.at[1], ar.at[1], device(z, x, c, y, down)))
    for t in zpeer:
        go(remote(ag.at[0, z], ag.at[0, z], bs.at[0, t], br.at[0, z], device(t, x, c, y, k)))

    for t in far_quad:
        part = kvb.at[t, x, c]
        remote(part, part, zs.at[t], zr.at[t], here).wait_recv()
        for u in xpeer:
            go(remote(part, part, xs.at[t, u], xr.at[t, x], device(z, u, c, y, k)))

    near = jnp.where((k == 0) | (k == 3), 2, 1)
    both = (near, 3 - near)
    for s in both:
        part = wall.at[y, pl.ds(pl.multiple_of(256 + 256 * s, 256), 256)]
        remote(part, part, w1s.at[s - 1], w1r.at[s - 1], here).wait_recv()
        for t in ypeer:
            go(remote(part, part, w2s.at[s, t], w2r.at[s, y], device(z, x, c, t, k)))
        remote(ag.at[0, z], ag.at[s, z], as_.at[s - 1], ar.at[s - 1], here).wait_recv()
        for t in zpeer:
            go(remote(ag.at[s, z], ag.at[s, z], bs.at[s, t], br.at[s, z], device(t, x, c, y, k)))

    for u in xpeer:
        for t in range(NZ):
            part = kvb.at[t, u, c]
            remote(part, part, xs.at[t, u], xr.at[t, u], here).wait_recv()
    own = kvb.at[:, :, c]
    go(remote(own, own, cs, cr, device(z, x, 1 - c, y, k)))

    def prefix():
        other = kvb.at[:, :, 1 - c]
        remote(other, other, cs, cr, here).wait_recv()
        load_t.wait()
        proj[...] = jnp.zeros_like(proj)

        @pl.loop(0, 8)
        def _(i):
            lhs = tokv[:, pl.ds(pl.multiple_of(i * 1024, 1024), 1024)]
            rhs = kvb[i].reshape(1024, 128)
            proj[...] += jnp.dot(lhs, rhs, preferred_element_type=jnp.float32)

        is_key = gy < KEY_VALUE_HEADS
        for i in range(plen.shape[0]):
            rows = slice(i * SLOT, (i + 1) * SLOT)
            plain = proj[rows]
            turned = plain * cos_t[rows] + pltpu.roll(plain, 64, 1) * sin_t[rows]
            kept = jnp.where(slot < plen[i], jnp.where(is_key, turned, plain), 0.0)
            kv_out[rows] = kept.astype(jnp.bfloat16)

    @pl.when(k == 0)
    def _():
        prefix()

    for t in ypeer:
        part = wall.at[t, pl.ds(0, 512)]
        remote(part, part, w2s.at[0, t], w2r.at[0, t], here).wait_recv()
        for s in (1, 2):
            part = wall.at[t, pl.ds(256 + 256 * s, 256)]
            remote(part, part, w2s.at[s, t], w2r.at[s, t], here).wait_recv()

    row16 = lax.broadcasted_iota(jnp.int32, (16, 128), 0) % 8

    def tiles(s):
        for t in zpeer:
            remote(ag.at[s, t], ag.at[s, t], bs.at[s, t], br.at[s, t], here).wait_recv()

    def picked(s, yy, zh, r):
        tile = ag[s, 2 * yy + zh // 2].astype(jnp.float32)
        return jnp.where(row16 == (zh % 2) * 4 + r, tile, 0.0).astype(jnp.bfloat16)

    def folded(s, acc):
        pair = [jnp.sum(acc[0:8], axis=0, keepdims=True), jnp.sum(acc[8:16], axis=0, keepdims=True)]
        obuf[s] = jnp.concatenate(pair + [jnp.zeros((6, 128), jnp.float32)], axis=0)

    def project(s):
        tiles(s)
        acc = jnp.zeros((16, 128), jnp.float32)
        parts = (
            (k, jnp.where(s == 1, 0, 2), jnp.where(s == 1, 0, 256)),
            (jnp.where(s == 1, up, down), jnp.where(s == 1, 2, 0), jnp.where(s == 1, 768, 512)),
        )
        for yy in range(4):
            for zh, r, lo in parts:
                lhs = jnp.concatenate([picked(s, yy, zh, r), picked(s, yy, zh, r + 1)], axis=1)
                rhs = wall[yy, pl.ds(pl.multiple_of(lo, 256), 256)]
                acc += jnp.dot(lhs, rhs, preferred_element_type=jnp.float32)
        folded(s, acc)
        to = device(z, x, c, y, (k + 5 - 2 * s) % 4)
        go(remote(obuf.at[s], rob.at[s - 1], os_.at[s - 1], or_.at[s - 1], to))

    project(both[0])
    tiles(0)
    acc = jnp.zeros((16, 128), jnp.float32)
    for yy in range(4):
        heads = [(k, r) for r in range(4)] + [(down, 0), (down, 1), (up, 2), (up, 3)]
        lhs = jnp.concatenate([picked(0, yy, zh, r) for zh, r in heads], axis=1)
        acc += jnp.dot(lhs, wall[yy], preferred_element_type=jnp.float32)
    folded(0, acc)

    project(both[1])

    @pl.when(k > 0)
    def _():
        prefix()

    for i in range(2):
        remote(obuf.at[i + 1], rob.at[i], os_.at[i], or_.at[i], here).wait_recv()
    dec[...] = (obuf[0, 0:2] + rob[0, 0:2] + rob[1, 0:2]).astype(jnp.bfloat16)
    for s in sends:
        s.wait_send()


def shards(tok, kvw, prefix_lengths, start_offsets, q, cache, lens, w):
    bf, f32 = jnp.bfloat16, jnp.float32
    vm = pltpu.VMEM
    dma = pltpu.SemaphoreType.DMA
    hbm = pl.BlockSpec(memory_space=pltpu.HBM)
    smem = pl.BlockSpec(memory_space=pltpu.SMEM)
    vmem = pl.BlockSpec(memory_space=pltpu.VMEM)
    inverse = rope_base ** (-2.0 * (np.arange(128) % 64) / HEAD_SIZE)
    prefix_kv, dec = pl.pallas_call(
        kernel,
        out_shape=(jax.ShapeDtypeStruct((tok.shape[0], 128), bf), jax.ShapeDtypeStruct((2, 128), bf)),
        in_specs=[smem] * 3 + [vmem] + [hbm] * 5,
        out_specs=(vmem, vmem),
        scratch_shapes=[
            vm((tok.shape[0], 128), f32), vm((tok.shape[0], 128), f32), vm((tok.shape[0], 128), f32),
            vm(tok.shape, bf), vm((8, 4, 2, 128, 128), bf), vm(q.shape, bf), vm(cache.shape, bf),
            vm((4, 1024, 128), bf), vm((8, 16, 256), bf), vm((8, 16, 256), bf), vm((16, 384), bf),
            vm((8, 16, 384), bf), vm((3, 8, 16, 128), bf), vm((3, 8, 128), f32), vm((2, 8, 128), f32),
            dma((5,)), dma((8,)), dma((8,)), dma((8,)), dma((8,)), dma((2,)), dma((2,)),
            dma((3, 8)), dma((3, 8)), dma((2,)), dma((2,)), dma((3, 4)), dma((3, 4)),
            dma((8,)), dma((8,)), dma((8, 4)), dma((8, 4)), dma, dma, dma((2,)), dma((2,)),
            pltpu.SemaphoreType.REGULAR((2,)),
        ],
        compiler_params=pltpu.CompilerParams(
            collective_id=0, has_side_effects=True, vmem_limit_bytes=67043328
        ),
    )(lens, prefix_lengths, start_offsets, np.float32(inverse)[None, :], tok, kvw, q, cache, w)
    return prefix_kv, dec


def solution(mesh):
    return jax.shard_map(
        shards,
        mesh=mesh,
        in_specs=(
            P("gx", None), P("gx", "gy"), P("gx"), P("gx"), P("gy", None),
            P(None, "gy", "gx", None), P("gy"), P("gy", "gx"),
        ),
        out_specs=(P("gx", "gy"), P("gy", "gx")),
        check_vma=False,
    )
```
